32 devices in a mesh: row: 4 (over y, x), col: 8 (over z, core).
Axes of the slice: x: 2, y: 2, z: 4, core: 2. Of those that a mesh axis runs over, the one named last changes fastest.
Arguments:
- amplitudes: bfloat16 [800, 800, 768], P('row', 'col'), may hold values from -6 to 6
- integrals: bfloat16 [800, 800, 256], P('row', 'col'), may hold values from -0.375 to 0.375
- window_index: int32 [256], replicated, may hold values from 0 to 639999, as said below
Outputs:
- residual: bfloat16 [800, 800, 768], P('row', 'col')
- pair_energy: float32 [768], replicated
The draws below stay inside these ranges and needn't reach their ends.
Inputs may be any that keep to these rules, and one draw needn't show every extreme that they name: `window_index`: the window pairs are distinct; pair k lies in the block of a rows and b columns owned by device number k // 8 in row-major order of the (a, b) device grid, 8 pairs for each block.
All inputs are finite; a program needn't handle non-finite values.
Results may differ from the reference program's by a relative error of at most 0.001.
Values may be sent and summed in bfloat16 or wider, within the bound.
A program may use at most 256 MiB of HBM per device.

```python
import jax
import jax.numpy as jnp
from jax import lax

VIRT = 800
PAIRS = 768
KD = 8
WINDOW = 256
N_ROW = 4
N_COL = 8


def draw_window_index(key, part):
    block_rows = VIRT // N_ROW
    block_cols = VIRT // N_COL
    device_keys = jax.random.split(jax.random.fold_in(key, 17), N_ROW * N_COL)

    def choose_cells(one_key):
        return jax.random.permutation(one_key, block_rows * block_cols)[:KD].astype(jnp.int32)
    picked = jax.vmap(choose_cells)(device_keys)
    device_ids = jnp.arange(N_ROW * N_COL, dtype=jnp.int32)
    row_ids = device_ids // N_COL
    col_ids = device_ids % N_COL
    a_index = row_ids[:, None] * block_rows + picked // block_cols
    b_index = col_ids[:, None] * block_cols + picked % block_cols
    return (a_index * VIRT + b_index).reshape(-1).astype(jnp.int32)


def level_of(stream_key, extent, pieces, least, high):
    level = 1.0
    for dim, blocks in pieces:
        draws = jax.random.uniform(jax.random.fold_in(jax.random.fold_in(stream_key, 6), dim), (blocks,), jnp.float32, least / len(pieces), high / len(pieces))
        level = level * jnp.repeat(jnp.exp(draws), extent[dim] // blocks).reshape((-1,) + (1,) * (len(extent) - 1 - dim))
    return level


def gaussian(key, shape, width, most, pieces=(), kind=jnp.bfloat16):
    entries = jax.random.normal(key, shape, jnp.float32) * width
    if len(pieces) > 0:
        entries = level_of(key, shape, pieces, -0.22, 0.18) * entries
    return jnp.clip(entries, min=-most, max=most).astype(kind)


def setup_inputs(seed: int = 0) -> dict:
    seeds = jax.random.split(jax.random.key(seed), 4)
    amplitudes = gaussian(seeds[0], (VIRT, VIRT, PAIRS), 1.0, 6.0, ((0, 4), (1, 8)))
    integrals = gaussian(seeds[1], (VIRT, VIRT, WINDOW), WINDOW ** -0.5, 0.375, ((0, 4), (1, 8)))
    window_index = draw_window_index(jax.random.fold_in(seeds[3], 71), 0)
    return dict(amplitudes=amplitudes, integrals=integrals, window_index=window_index)


def reference(amplitudes, integrals, window_index):
    flattened = amplitudes.reshape(VIRT * VIRT, PAIRS)
    columns = jnp.take(flattened, window_index, axis=0)
    block_rows = VIRT // N_ROW

    def one_block(block_index):
        start = (block_index * block_rows).astype(jnp.int32)
        part_ints = lax.dynamic_slice_in_dim(integrals, start, block_rows, 0)
        part_amps = lax.dynamic_slice_in_dim(amplitudes, start, block_rows, 0)
        full = jnp.dot(part_ints.reshape(block_rows * VIRT, WINDOW), columns, preferred_element_type=jnp.float32)
        energy = jnp.sum(part_amps.reshape(block_rows * VIRT, PAIRS).astype(jnp.float32) * full, axis=0)
        return full.astype(jnp.bfloat16), energy

    blocks, energies = lax.map(one_block, jnp.arange(N_ROW, dtype=jnp.int32))
    residual = blocks.reshape(VIRT, VIRT, PAIRS)
    pair_energy = jnp.sum(energies, axis=0) / VIRT
    return residual, pair_energy
```

```python
import functools

import jax
import jax.numpy as jnp
from jax import lax
from jax.experimental import pallas as pl
from jax.experimental.pallas import tpu as pltpu
from jax.sharding import PartitionSpec as P

MESH = pl.DeviceIdType.MESH


def exchange_kernel(nrows, ncols, own_ref, out_ref, send_sems, recv_sems):
    count = nrows * ncols
    me = lax.axis_index("row") * ncols + lax.axis_index("col")

    def place(step):
        other = lax.rem(me + step, count)
        return (other // ncols, lax.rem(other, ncols))

    barrier = pltpu.get_barrier_semaphore()

    def greet(step, carry):
        pl.semaphore_signal(barrier, inc=1, device_id=place(step), device_id_type=MESH)
        return carry

    lax.fori_loop(1, count, greet, 0)
    pl.semaphore_wait(barrier, count - 1)

    def copy(step, slot):
        return pltpu.make_async_remote_copy(
            src_ref=own_ref,
            dst_ref=out_ref.at[slot],
            send_sem=send_sems.at[step],
            recv_sem=recv_sems.at[step],
            device_id=place(step),
            device_id_type=MESH,
        )

    def send(step, carry):
        copy(step, me).start()
        return carry

    lax.fori_loop(1, count, send, 0)
    out_ref[me] = own_ref[...]

    def finish(step, carry):
        source = lax.rem(me + count - step, count)
        copy(step, source).wait_recv()
        copy(step, me).wait_send()
        return carry

    lax.fori_loop(1, count, finish, 0)


def exchange(block, nrows, ncols, collective_id):
    count = nrows * ncols
    return pl.pallas_call(
        functools.partial(exchange_kernel, nrows, ncols),
        out_shape=jax.ShapeDtypeStruct((count,) + block.shape, block.dtype),
        in_specs=[pl.BlockSpec(memory_space=pltpu.VMEM)],
        out_specs=pl.BlockSpec(memory_space=pltpu.VMEM),
        scratch_shapes=[
            pltpu.SemaphoreType.DMA((count,)),
            pltpu.SemaphoreType.DMA((count,)),
        ],
        compiler_params=pltpu.CompilerParams(collective_id=collective_id, has_side_effects=True),
    )(block)


ROWS = 2000
SUB = 200


def largest_divisor(extent, most, multiple):
    fits = [d for d in range(multiple, min(extent, most) + 1, multiple) if extent % d == 0]
    return max(fits) if fits else extent


def ladder_kernel(sub, chunk, amps_ref, ints_ref, cols_ref, residual_ref, energy_ref, total_ref):
    rows, pairs = amps_ref.shape

    @pl.when(pl.program_id(0) == 0)
    def _():
        total_ref[...] = jnp.zeros_like(total_ref)

    for start in range(0, pairs, chunk):
        span = slice(start, start + chunk)
        total = jnp.zeros((8, chunk), jnp.float32)
        for low in range(0, rows, sub):
            part = slice(low, low + sub)
            full = jnp.dot(ints_ref[part], cols_ref[:, span], preferred_element_type=jnp.float32)
            residual_ref[part, span] = full.astype(residual_ref.dtype)
            weighted = amps_ref[part, span].astype(jnp.float32) * full
            total = total + jnp.sum(weighted.reshape(sub // 8, 8, chunk), axis=0)
        total_ref[:, span] += total

    @pl.when(pl.program_id(0) == pl.num_programs(0) - 1)
    def _():
        energy_ref[...] = jnp.sum(total_ref[...], axis=0, keepdims=True)


def ladder(amplitudes, integrals, columns):
    cells, pairs = amplitudes.shape
    window = integrals.shape[1]
    rows = largest_divisor(cells, ROWS, 8)
    sub = largest_divisor(rows, SUB, 8)
    chunk = 256 if pairs % 256 == 0 else pairs
    return pl.pallas_call(
        functools.partial(ladder_kernel, sub, chunk),
        grid=(cells // rows,),
        out_shape=(
            jax.ShapeDtypeStruct((cells, pairs), jnp.bfloat16),
            jax.ShapeDtypeStruct((1, pairs), jnp.float32),
        ),
        in_specs=[
            pl.BlockSpec((rows, pairs), lambda i: (i, 0)),
            pl.BlockSpec((rows, window), lambda i: (i, 0)),
            pl.BlockSpec((window, pairs), lambda i: (0, 0)),
        ],
        out_specs=(
            pl.BlockSpec((rows, pairs), lambda i: (i, 0)),
            pl.BlockSpec((1, pairs), lambda i: (0, 0)),
        ),
        scratch_shapes=[pltpu.VMEM((8, pairs), jnp.float32)],
        compiler_params=pltpu.CompilerParams(
            dimension_semantics=("arbitrary",), vmem_limit_bytes=60 * 1024 * 1024
        ),
    )(amplitudes, integrals, columns)


def shards(amplitudes, integrals, window_index):
    block_rows, block_cols, pairs = amplitudes.shape
    window = integrals.shape[2]
    ncols = lax.axis_size("col")
    nrows = lax.axis_size("row")
    per_device = window // (nrows * ncols)
    row_rank = lax.axis_index("row")
    col_rank = lax.axis_index("col")
    linear_rank = row_rank * ncols + col_rank
    owned_index = lax.dynamic_slice_in_dim(window_index, linear_rank * per_device, per_device)
    virtuals = block_rows * nrows
    row_offset = owned_index // virtuals - row_rank * block_rows
    col_offset = owned_index % virtuals - col_rank * block_cols
    owned = amplitudes[row_offset, col_offset]
    columns = exchange(owned, nrows, ncols, 0).reshape(window, pairs)
    cells = block_rows * block_cols
    residual, partial_value = ladder(
        amplitudes.transpose(1, 0, 2).reshape(cells, pairs),
        integrals.transpose(1, 0, 2).reshape(cells, window),
        columns,
    )
    residual = residual.reshape(block_cols, block_rows, pairs).transpose(1, 0, 2)
    values = exchange(partial_value, nrows, ncols, 1)
    pair_energy = jnp.sum(values[:, 0, :], axis=0) / virtuals
    return (residual, pair_energy)


def solution(mesh):
    return jax.shard_map(
        shards,
        mesh=mesh,
        in_specs=(P("row", "col", None), P("row", "col", None), P()),
        out_specs=(P("row", "col", None), P()),
        check_vma=False,
    )
```
